32 devices in a mesh: energy: 8 (over z, x), slab: 4 (over y, core).
Axes of the slice: x: 2, y: 2, z: 4, core: 2. Of those that a mesh axis runs over, the one named last changes fastest.
Arguments:
- green_blocks: bfloat16 [8, 4, 512, 512], P('energy', 'slab'), may hold values from -6 to 6
- coulomb: bfloat16 [4, 512, 512], P('slab'), may hold values from -0.25 to 0.25
- couple_cols: int32 [4, 128, 8], P('slab'), may hold values from 0 to 127
- couple_vals: bfloat16 [4, 128, 8], P('slab'), may hold values from -0.8984375 to 0.8984375
Outputs:
- new_green: bfloat16 [8, 4, 512, 512], P('energy', 'slab')
The draws below stay inside these ranges and needn't reach their ends.
Inputs may be any that keep to these rules, and one draw needn't show every extreme that they name: couple_cols[s, i, k] names one of the first 128 orbitals of slab s + 1.
All inputs are finite; a program needn't handle non-finite values.
Results may differ from the reference program's by a relative error of at most 0.015.
Values may be sent and summed in bfloat16 or wider, within the bound.
A program may use at most 64 MiB of HBM per device.

```python
import math
import jax
import jax.numpy as jnp
from jax import lax

M = 512
COUPLINGS = 8
IFACE = 128
NE = 8
SLABS = 4


def with_ends(values, own_key, least, high):
    spot = [jax.random.randint(jax.random.fold_in(own_key, axis), (), 0, length) for axis, length in enumerate(values.shape)]
    main_axis = values.shape.index(max(values.shape))
    neighbour = spot[:main_axis] + [(spot[main_axis] + 1) % values.shape[main_axis]] + spot[main_axis + 1:]
    return values.at[tuple(spot)].set(least).at[tuple(neighbour)].set(high)


def block_scale(own_key, dims, split, low, largest):
    factor_of = 1.0
    for position, shards_of in split:
        steps = jax.random.uniform(jax.random.fold_in(jax.random.fold_in(own_key, 6), position), (shards_of,), jnp.float32, low / len(split), largest / len(split))
        factor_of = factor_of * jnp.repeat(jnp.exp(steps), dims[position] // shards_of).reshape((-1,) + (1,) * (len(dims) - 1 - position))
    return factor_of


def bell_draw(rng, shape, deviation, bound, cuts=(), kind=jnp.bfloat16):
    array = jax.random.normal(rng, shape, jnp.float32) * deviation
    if len(cuts) > 0:
        array = block_scale(rng, shape, cuts, -0.22, 0.18) * array
    return jnp.clip(array, min=-bound, max=bound).astype(kind)


def setup_inputs(seed: int = 0) -> dict:
    streams_of = jax.random.split(jax.random.key(seed), 5)
    green_blocks = bell_draw(streams_of[0], (NE, SLABS, M, M), 1.0, 6.0, ((0, 8), (1, 4)))
    coulomb = bell_draw(streams_of[1], (SLABS, M, M), M ** -0.5, 0.25, ((0, 4),))
    couple_cols = with_ends(jax.random.randint(streams_of[2], (SLABS, IFACE, COUPLINGS), 0, IFACE), jax.random.fold_in(streams_of[2], 1), 0, IFACE - 1).astype(jnp.int32)
    couple_vals = bell_draw(streams_of[3], (SLABS, IFACE, COUPLINGS), 0.15, 0.8984375, ((0, 4),))
    return dict(green_blocks=green_blocks, coulomb=coulomb, couple_cols=couple_cols, couple_vals=couple_vals)


row_block = 32

def coupling_matrix(column_ids, coupling_values):
    width = column_ids.shape[0]
    hits = column_ids[:, :, None] == jnp.arange(width, dtype=jnp.int32)[None, None, :]
    summed = lax.optimization_barrier(jnp.sum(jnp.where(hits, coupling_values.astype(jnp.float32)[:, :, None], jnp.float32(0.0)), axis=1))
    return summed.astype(jnp.bfloat16)

def screen(polar_one, coulomb_block):
    inner = jnp.dot(coulomb_block, polar_one, preferred_element_type=jnp.float32).astype(jnp.bfloat16)
    second = jnp.dot(inner, coulomb_block, preferred_element_type=jnp.float32)
    third = jnp.dot(inner, second.astype(jnp.bfloat16), preferred_element_type=jnp.float32)
    return (coulomb_block.astype(jnp.float32) + second + third).astype(jnp.bfloat16)

def batched(left, right):
    return jnp.einsum('eij,ejk->eik', left.astype(jnp.float32), right.astype(jnp.float32))

def reference(green_blocks, coulomb, couple_cols, couple_vals):
    inv_root = 1.0 / math.sqrt(M)
    block_starts = jnp.arange(M // row_block, dtype=jnp.int32) * row_block
    outputs = []
    for slab_index in range(SLABS):
        green_slab = green_blocks[:, slab_index]
        coulomb_block = coulomb[slab_index]

        def polar_rows(start):
            rows_now = lax.dynamic_slice_in_dim(green_slab, start, row_block, 1).astype(jnp.float32)
            mirror = jnp.swapaxes(lax.dynamic_slice_in_dim(green_slab, start, row_block, 2), 1, 2).astype(jnp.float32)
            spectra = jnp.fft.fft(rows_now, axis=0) * jnp.conj(jnp.fft.fft(mirror, axis=0))
            return jnp.real(jnp.fft.ifft(spectra, axis=0)).astype(jnp.float32)
        polar = jnp.swapaxes(lax.map(polar_rows, block_starts), 0, 1).reshape(NE, M, M)
        polar = (polar * (0.5 / math.sqrt(M * NE))).astype(jnp.bfloat16)
        screened = lax.map(lambda polar_one: screen(polar_one, coulomb_block), polar)
        screened = lax.optimization_barrier(screened)

        def sigma_rows(start):
            rows_now = lax.dynamic_slice_in_dim(green_slab, start, row_block, 1).astype(jnp.float32)
            waves = lax.dynamic_slice_in_dim(screened, start, row_block, 1).astype(jnp.float32)
            spectra = jnp.fft.fft(rows_now, axis=0) * jnp.fft.fft(waves, axis=0)
            return jnp.real(jnp.fft.ifft(spectra, axis=0)).astype(jnp.float32)
        sigma = jnp.swapaxes(lax.map(sigma_rows, block_starts), 0, 1).reshape(NE, M, M)
        sigma = (sigma * (0.2 / math.sqrt(NE))).astype(jnp.bfloat16)
        total = sigma.astype(jnp.float32)
        last = M - IFACE
        if slab_index + 1 < SLABS:
            coupling = coupling_matrix(couple_cols[slab_index], couple_vals[slab_index])
            corner = green_blocks[:, slab_index + 1, :IFACE, :IFACE]
            near_next = jnp.einsum('ij,ejk->eik', coupling.astype(jnp.float32), corner.astype(jnp.float32))
            near_next = lax.optimization_barrier(near_next.astype(jnp.bfloat16))
            right_part = jnp.einsum('eij,kj->eik', near_next.astype(jnp.float32), coupling.astype(jnp.float32)) * inv_root
            total = total.at[:, last:, last:].add(right_part)
        if slab_index > 0:
            previous = coupling_matrix(couple_cols[slab_index - 1], couple_vals[slab_index - 1])
            corner = green_blocks[:, slab_index - 1, last:, last:]
            near_prev = jnp.einsum('ji,ejk->eik', previous.astype(jnp.float32), corner.astype(jnp.float32))
            near_prev = lax.optimization_barrier(near_prev.astype(jnp.bfloat16))
            left_part = jnp.einsum('eij,jk->eik', near_prev.astype(jnp.float32), previous.astype(jnp.float32)) * inv_root
            total = total.at[:, :IFACE, :IFACE].add(left_part)
        total_b = lax.optimization_barrier(total.astype(jnp.bfloat16))
        dressed = lax.optimization_barrier(batched(green_slab, total_b).astype(jnp.bfloat16))
        updated = green_slab.astype(jnp.float32) + batched(dressed, green_slab) * inv_root
        outputs.append(updated.astype(jnp.bfloat16))
    return jnp.stack(outputs, axis=1)
```

```python
import functools
import math

import jax
import jax.numpy as jnp
from jax import lax
from jax.experimental import pallas as pl
from jax.experimental.pallas import tpu as pltpu
from jax.sharding import PartitionSpec as P


def from_behind(x, axis, by):
    size = lax.axis_size(axis)
    pairs = [(i, i + by) for i in range(size) if 0 <= i + by < size]
    return lax.ppermute(x, axis, pairs)


def plain_dot(left, right):
    return jnp.dot(left, right, preferred_element_type=jnp.float32)


def split_parts(values):
    upper = values.astype(jnp.bfloat16)
    lower = (values - upper.astype(jnp.float32)).astype(jnp.bfloat16)
    return (upper, lower)


def coupling_matrix(column_ids, coupling_values):
    width = column_ids.shape[0]
    hits = column_ids[:, :, None] == jnp.arange(width, dtype=jnp.int32)[None, None, :]
    summed = jnp.sum(
        jnp.where(hits, coupling_values.astype(jnp.float32)[:, :, None], jnp.float32(0.0)), axis=1
    )
    return summed.astype(jnp.bfloat16)


def on_device(green_blocks, coulomb, couple_cols, couple_vals):
    own_green = green_blocks[:, 0]
    coulomb_block = coulomb[0]
    per_device = own_green.shape[0]
    orbitals = own_green.shape[1]
    volume = lax.axis_size("energy")
    energies = per_device * volume
    inv_root = 1.0 / math.sqrt(orbitals)
    flipped = jnp.swapaxes(own_green, 1, 2)
    received, flipped_recv = (
        lax.all_to_all(own_green, "energy", split_axis=1, concat_axis=0, tiled=True),
        lax.all_to_all(flipped, "energy", split_axis=1, concat_axis=0, tiled=True),
    )
    green_entries = received.reshape(energies, -1)
    flipped_entries = flipped_recv.reshape(energies, -1)
    entry_shape = received.shape
    halfway = energies // 2 + 1
    frequency = jnp.arange(halfway, dtype=jnp.int32)
    energy_index = jnp.arange(energies, dtype=jnp.int32)
    angles = (frequency[:, None] * energy_index[None, :] % energies).astype(jnp.float32) * (
        2.0 * math.pi / energies
    )
    cosine = jnp.cos(angles)
    sine = jnp.sin(angles)
    weights = (
        jnp.where((frequency == 0) | (2 * frequency == energies), 1.0, 2.0).astype(jnp.float32)
        / energies
    )
    forward_high, forward_low = split_parts(jnp.concatenate([cosine, -sine], axis=0))
    backward_table = jnp.concatenate(
        [cosine * weights[:, None], -sine * weights[:, None]], axis=0
    ).T
    backward_high, backward_low = split_parts(backward_table)

    def spectrum(entries):
        stacked = plain_dot(forward_high, entries) + plain_dot(forward_low, entries)
        return (stacked[:halfway], stacked[halfway:])

    def to_values(real_part, imag_part):
        data_high, data_low = split_parts(jnp.concatenate([real_part, imag_part], axis=0))
        return (
            plain_dot(backward_high, data_high)
            + plain_dot(backward_high, data_low)
            + plain_dot(backward_low, data_high)
        )

    green_real, green_imag = spectrum(green_entries)
    mirror_real, mirror_imag = spectrum(flipped_entries)
    polar_entries = to_values(
        green_real * mirror_real + green_imag * mirror_imag,
        green_imag * mirror_real - green_real * mirror_imag,
    )
    polar_entries = (polar_entries * (0.5 / math.sqrt(orbitals * energies))).astype(jnp.bfloat16)
    polar = lax.all_to_all(
        polar_entries.reshape(entry_shape), "energy", split_axis=0, concat_axis=1, tiled=True
    )
    inner = jnp.einsum(
        "ij,ejk->eik", coulomb_block, polar, preferred_element_type=jnp.float32
    ).astype(jnp.bfloat16)
    second = jnp.einsum("eij,jk->eik", inner, coulomb_block, preferred_element_type=jnp.float32)
    third = jnp.einsum(
        "eij,ejk->eik", inner, second.astype(jnp.bfloat16), preferred_element_type=jnp.float32
    )
    screened = (coulomb_block.astype(jnp.float32)[None] + second + third).astype(jnp.bfloat16)
    screened_entries = lax.all_to_all(
        screened, "energy", split_axis=1, concat_axis=0, tiled=True
    ).reshape(energies, -1)
    screen_real, screen_imag = spectrum(screened_entries)
    sigma_entries = to_values(
        green_real * screen_real - green_imag * screen_imag,
        green_real * screen_imag + green_imag * screen_real,
    )
    sigma_entries = (sigma_entries * (0.2 / math.sqrt(energies))).astype(jnp.bfloat16)
    sigma = lax.all_to_all(
        sigma_entries.reshape(entry_shape), "energy", split_axis=0, concat_axis=1, tiled=True
    )
    interface = couple_cols.shape[1]
    last = orbitals - interface
    coupling = coupling_matrix(couple_cols[0], couple_vals[0])
    prev_green, previous = from_behind((own_green, coupling), "slab", 1)
    next_green = from_behind(own_green, "slab", -1)
    prev_corner = prev_green[:, last:, last:]
    next_corner = next_green[:, :interface, :interface]
    near_next = jnp.einsum(
        "ij,ejk->eik", coupling, next_corner, preferred_element_type=jnp.float32
    ).astype(jnp.bfloat16)
    near_prev = jnp.einsum(
        "ji,ejk->eik", previous, prev_corner, preferred_element_type=jnp.float32
    ).astype(jnp.bfloat16)
    right_part = (
        jnp.einsum("eij,kj->eik", near_next, coupling, preferred_element_type=jnp.float32)
        * inv_root
    )
    left_part = (
        jnp.einsum("eij,jk->eik", near_prev, previous, preferred_element_type=jnp.float32)
        * inv_root
    )
    total = sigma.astype(jnp.float32)
    total = total.at[:, last:, last:].add(right_part)
    total = total.at[:, :interface, :interface].add(left_part)
    total_b = total.astype(jnp.bfloat16)
    dressed = jnp.einsum(
        "eij,ejk->eik", own_green, total_b, preferred_element_type=jnp.float32
    ).astype(jnp.bfloat16)
    updated = (
        own_green
        + jnp.einsum("eij,ejk->eik", dressed, own_green, preferred_element_type=jnp.float32)
        * inv_root
    )
    return updated.astype(jnp.bfloat16)[:, None]


MESH = pl.DeviceIdType.MESH


def unit_blocks(unit, grid):
    odd = grid - 1
    paired = grid * odd // 2
    slot = unit // odd
    turn = unit % odd
    diagonal = unit // paired
    first = (turn + slot) % odd
    second = (turn + odd - slot) % odd
    lone = 1 - (slot + odd - 1) // odd
    row = lone * odd + (1 - lone) * first
    col = lone * turn + (1 - lone) * second
    corner = 2 * (unit - paired)
    row0 = diagonal * corner + (1 - diagonal) * row
    col0 = diagonal * corner + (1 - diagonal) * col
    row1 = diagonal * (corner + 1) + (1 - diagonal) * col
    col1 = diagonal * (corner + 1) + (1 - diagonal) * row
    return ((row0, col0), (row1, col1))


def fused_kernel(
    volume, slabs, grid, scale_polar, scale_sigma, inv_root,
    green, coulomb, cols, vals, out,
    green_in, mirror, polar_out, polar_in, matrix, inner, screened, screen_in, sigma_out, sigma_in,
    coupling, turned, next_corner, left_out, left_in, total,
    send_sem, recv_sem, slab_send, slab_recv,
):
    me = lax.axis_index("energy")
    slab = lax.axis_index("slab")
    size = green.shape[0] // grid
    last = green.shape[0] - size
    order = sorted(range(1, volume), key=lambda k: (-min(k, volume - k), k))
    has_prev = 1 - (slabs - 1 - slab + 0) // (slabs - 1)
    has_next = 1 - slab // (slabs - 1)
    diagonal = me // (grid * (grid - 1) // 2)

    def peer_of(k):
        return lax.rem(me + k, volume)

    barrier = pltpu.get_barrier_semaphore()
    for k in range(1, volume):
        pl.semaphore_signal(barrier, inc=1, device_id=(peer_of(k), slab), device_id_type=MESH)

    @pl.when(slab > 0)
    def _():
        pl.semaphore_signal(barrier, inc=1, device_id=(me, slab - 1), device_id_type=MESH)

    @pl.when(slab < slabs - 1)
    def _():
        pl.semaphore_signal(barrier, inc=1, device_id=(me, slab + 1), device_id_type=MESH)

    pl.semaphore_wait(barrier, volume - 1 + has_prev + has_next)

    def block_of(ref, coords):
        row = pl.multiple_of(coords[0] * size, size)
        col = pl.multiple_of(coords[1] * size, size)
        return ref.at[pl.ds(row, size), pl.ds(col, size)]

    def remote(src, dst, phase, k, half):
        return pltpu.make_async_remote_copy(
            src_ref=src, dst_ref=dst,
            send_sem=send_sem.at[phase, k, half], recv_sem=recv_sem.at[phase, k, half],
            device_id=(peer_of(k), slab), device_id_type=MESH,
        )

    def scatter(source, landing, phase):
        copies = []
        for k in order:
            coords = unit_blocks(peer_of(k), grid)
            for half in range(2):
                copy = remote(block_of(source, coords[half]), landing.at[me, half], phase, k, half)
                copy.start()
                copies.append(copy)
        own = unit_blocks(me, grid)
        for half in range(2):
            landing[me, half] = block_of(source, own[half])[...]
        return copies

    def gather(source, landing, phase, half):
        copies = []
        for k in order:
            copy = remote(source.at[peer_of(k), half], landing.at[me, half], phase, k, half)
            copy.start()
            copies.append(copy)
        landing[me, half] = source[me, half]
        return copies

    def arrived(copies):
        for copy in copies:
            copy.wait_recv()

    def assemble(landing, target):
        for unit in range(volume):
            coords = unit_blocks(unit, grid)
            for half in range(2):
                row, col = coords[half]
                target[row * size:(row + 1) * size, col * size:(col + 1) * size] = landing[unit, half]

    sent = scatter(green, green_in, 0)
    corner_copy = pltpu.make_async_remote_copy(
        src_ref=green.at[pl.ds(0, size), pl.ds(0, size)], dst_ref=next_corner,
        send_sem=slab_send.at[0], recv_sem=slab_recv.at[0],
        device_id=(me, slab - has_prev), device_id_type=MESH,
    )
    left_copy = pltpu.make_async_remote_copy(
        src_ref=left_out, dst_ref=left_in,
        send_sem=slab_send.at[1], recv_sem=slab_recv.at[1],
        device_id=(me, slab + has_next), device_id_type=MESH,
    )

    @pl.when(slab > 0)
    def _():
        corner_copy.start()

    ids = cols[...]
    values = vals[...].astype(jnp.float32)
    columns = lax.broadcasted_iota(jnp.int32, (size, size), 1)
    summed = jnp.zeros((size, size), jnp.float32)
    for k in range(ids.shape[1]):
        summed += jnp.where(ids[:, k:k + 1] == columns, values[:, k:k + 1], jnp.float32(0.0))
    summed = summed.astype(jnp.bfloat16).astype(jnp.float32)
    coupling[...] = summed.astype(jnp.bfloat16)
    turned[...] = summed.T.astype(jnp.bfloat16)

    @pl.when(slab < slabs - 1)
    def _():
        near_prev = plain_dot(turned[...], green[last:, last:]).astype(jnp.bfloat16)
        left_out[...] = plain_dot(near_prev, coupling[...]) * inv_root
        left_copy.start()

    arrived(sent)
    everything = list(sent)
    rows_at_once = 16

    for half in range(2):
        other = diagonal * half + (1 - diagonal) * (1 - half)

        def flip(e, carry, half=half, other=other):
            mirror[e, half] = green_in[e, other].astype(jnp.float32).T
            return carry

        lax.fori_loop(0, volume, flip, 0)

    for half in range(2):
        def correlate(step, carry, half=half):
            rows = pl.ds(pl.multiple_of(step * rows_at_once, rows_at_once), rows_at_once)
            mine = [green_in[e, half, rows, :].astype(jnp.float32) for e in range(volume)]
            theirs = [mirror[e, half, rows, :] for e in range(volume)]
            for e in range(volume):
                acc = mine[0] * theirs[(0 - e) % volume]
                for e2 in range(1, volume):
                    acc += mine[e2] * theirs[(e2 - e) % volume]
                polar_out[e, half, rows, :] = (acc * scale_polar).astype(jnp.bfloat16)
            return carry

        lax.fori_loop(0, size // rows_at_once, correlate, 0)
        copies = gather(polar_out, polar_in, 1, half)
        everything += copies
        if half == 0:
            polar_copies = copies
        else:
            polar_copies = polar_copies + copies
    arrived(polar_copies)
    assemble(polar_in, matrix)
    inner[...] = plain_dot(coulomb[...], matrix[...]).astype(jnp.bfloat16)
    second = plain_dot(inner[...], coulomb[...])
    total[...] = second
    matrix[...] = second.astype(jnp.bfloat16)
    third = plain_dot(inner[...], matrix[...])
    screened[...] = (coulomb[...].astype(jnp.float32) + total[...] + third).astype(jnp.bfloat16)
    copies = scatter(screened, screen_in, 2)
    everything += copies
    arrived(copies)

    sigma_copies = []
    for half in range(2):
        def convolve(step, carry, half=half):
            rows = pl.ds(pl.multiple_of(step * rows_at_once, rows_at_once), rows_at_once)
            mine = [green_in[e, half, rows, :].astype(jnp.float32) for e in range(volume)]
            waves = [screen_in[e, half, rows, :].astype(jnp.float32) for e in range(volume)]
            for e in range(volume):
                acc = mine[0] * waves[e]
                for e2 in range(1, volume):
                    acc += mine[e2] * waves[(e - e2) % volume]
                sigma_out[e, half, rows, :] = (acc * scale_sigma).astype(jnp.bfloat16)
            return carry

        lax.fori_loop(0, size // rows_at_once, convolve, 0)
        sigma_copies += gather(sigma_out, sigma_in, 3, half)
    everything += sigma_copies
    arrived(sigma_copies)
    assemble(sigma_in, matrix)

    @pl.when(slab < slabs - 1)
    def _():
        corner_copy.wait_recv()
        near_next = plain_dot(coupling[...], next_corner[...]).astype(jnp.bfloat16)
        right_part = plain_dot(near_next, turned[...]) * inv_root
        matrix[last:, last:] = (matrix[last:, last:].astype(jnp.float32) + right_part).astype(jnp.bfloat16)
        left_copy.wait_send()

    @pl.when(slab > 0)
    def _():
        left_copy.wait_recv()
        matrix[:size, :size] = (matrix[:size, :size].astype(jnp.float32) + left_in[...]).astype(jnp.bfloat16)
        corner_copy.wait_send()

    inner[...] = plain_dot(green[...], matrix[...]).astype(jnp.bfloat16)
    updated = green[...].astype(jnp.float32) + plain_dot(inner[...], green[...]) * inv_root
    out[...] = updated.astype(jnp.bfloat16)
    for copy in everything:
        copy.wait_send()


def fused_on_device(grid, green_blocks, coulomb, couple_cols, couple_vals):
    volume = lax.axis_size("energy")
    slabs = lax.axis_size("slab")
    orbitals = green_blocks.shape[-1]
    size = orbitals // grid
    half_type = jnp.bfloat16
    pieces = pltpu.VMEM((volume, 2, size, size), half_type)
    whole = pltpu.VMEM((orbitals, orbitals), half_type)
    block = pltpu.VMEM((size, size), half_type)
    wide = pltpu.VMEM((size, size), jnp.float32)
    result = pl.pallas_call(
        functools.partial(
            fused_kernel, volume, slabs, grid,
            0.5 / math.sqrt(orbitals * volume), 0.2 / math.sqrt(volume), 1.0 / math.sqrt(orbitals),
        ),
        out_shape=jax.ShapeDtypeStruct((orbitals, orbitals), half_type),
        in_specs=[pl.BlockSpec(memory_space=pltpu.VMEM)] * 4,
        out_specs=pl.BlockSpec(memory_space=pltpu.VMEM),
        scratch_shapes=[
            pieces, pltpu.VMEM((volume, 2, size, size), jnp.float32), pieces, pieces,
            whole, whole, whole, pieces, pieces, pieces,
            block, block, block, wide, wide, pltpu.VMEM((orbitals, orbitals), jnp.float32),
            pltpu.SemaphoreType.DMA((4, volume, 2)), pltpu.SemaphoreType.DMA((4, volume, 2)),
            pltpu.SemaphoreType.DMA((2,)), pltpu.SemaphoreType.DMA((2,)),
        ],
        compiler_params=pltpu.CompilerParams(
            collective_id=0, has_side_effects=True, vmem_limit_bytes=40 * 2 ** 20
        ),
    )(green_blocks[0, 0], coulomb[0], couple_cols[0], couple_vals[0])
    return result[None, None]


def fused_grid(mesh):
    volume = mesh.shape["energy"]
    grid = math.isqrt(2 * volume)
    return grid if grid * grid == 2 * volume and grid % 2 == 0 else 0


def on_any(grid, green_blocks, coulomb, couple_cols, couple_vals):
    orbitals = green_blocks.shape[-1]
    fits = (
        grid > 0
        and green_blocks.shape[:2] == (1, 1)
        and orbitals % (128 * max(grid, 1)) == 0
        and couple_cols.shape[1] * grid == orbitals
        and lax.axis_size("slab") > 1
    )
    if fits:
        return fused_on_device(grid, green_blocks, coulomb, couple_cols, couple_vals)
    return on_device(green_blocks, coulomb, couple_cols, couple_vals)


def solution(mesh):
    return jax.shard_map(
        functools.partial(on_any, fused_grid(mesh)),
        mesh=mesh,
        in_specs=(
            P("energy", "slab", None, None),
            P("slab", None, None),
            P("slab", None, None),
            P("slab", None, None),
        ),
        out_specs=P("energy", "slab", None, None),
        check_vma=False,
    )
```

```python
import functools
import math

import jax
import jax.numpy as jnp
from jax import lax
from jax.experimental import pallas as pl
from jax.experimental.pallas import tpu as pltpu
from jax.sharding import PartitionSpec as P


def from_behind(x, axis, by):
    size = lax.axis_size(axis)
    pairs = [(i, i + by) for i in range(size) if 0 <= i + by < size]
    return lax.ppermute(x, axis, pairs)


def plain_dot(left, right):
    return jnp.dot(left, right, preferred_element_type=jnp.float32)


def split_parts(values):
    upper = values.astype(jnp.bfloat16)
    lower = (values - upper.astype(jnp.float32)).astype(jnp.bfloat16)
    return (upper, lower)


def coupling_matrix(column_ids, coupling_values):
    width = column_ids.shape[0]
    hits = column_ids[:, :, None] == jnp.arange(width, dtype=jnp.int32)[None, None, :]
    summed = jnp.sum(
        jnp.where(hits, coupling_values.astype(jnp.float32)[:, :, None], jnp.float32(0.0)), axis=1
    )
    return summed.astype(jnp.bfloat16)


def on_device(green_blocks, coulomb, couple_cols, couple_vals):
    own_green = green_blocks[:, 0]
    coulomb_block = coulomb[0]
    per_device = own_green.shape[0]
    orbitals = own_green.shape[1]
    volume = lax.axis_size("energy")
    energies = per_device * volume
    inv_root = 1.0 / math.sqrt(orbitals)
    flipped = jnp.swapaxes(own_green, 1, 2)
    received, flipped_recv = (
        lax.all_to_all(own_green, "energy", split_axis=1, concat_axis=0, tiled=True),
        lax.all_to_all(flipped, "energy", split_axis=1, concat_axis=0, tiled=True),
    )
    green_entries = received.reshape(energies, -1)
    flipped_entries = flipped_recv.reshape(energies, -1)
    entry_shape = received.shape
    halfway = energies // 2 + 1
    frequency = jnp.arange(halfway, dtype=jnp.int32)
    energy_index = jnp.arange(energies, dtype=jnp.int32)
    angles = (frequency[:, None] * energy_index[None, :] % energies).astype(jnp.float32) * (
        2.0 * math.pi / energies
    )
    cosine = jnp.cos(angles)
    sine = jnp.sin(angles)
    weights = (
        jnp.where((frequency == 0) | (2 * frequency == energies), 1.0, 2.0).astype(jnp.float32)
        / energies
    )
    forward_high, forward_low = split_parts(jnp.concatenate([cosine, -sine], axis=0))
    backward_table = jnp.concatenate(
        [cosine * weights[:, None], -sine * weights[:, None]], axis=0
    ).T
    backward_high, backward_low = split_parts(backward_table)

    def spectrum(entries):
        stacked = plain_dot(forward_high, entries) + plain_dot(forward_low, entries)
        return (stacked[:halfway], stacked[halfway:])

    def to_values(real_part, imag_part):
        data_high, data_low = split_parts(jnp.concatenate([real_part, imag_part], axis=0))
        return (
            plain_dot(backward_high, data_high)
            + plain_dot(backward_high, data_low)
            + plain_dot(backward_low, data_high)
        )

    green_real, green_imag = spectrum(green_entries)
    mirror_real, mirror_imag = spectrum(flipped_entries)
    polar_entries = to_values(
        green_real * mirror_real + green_imag * mirror_imag,
        green_imag * mirror_real - green_real * mirror_imag,
    )
    polar_entries = (polar_entries * (0.5 / math.sqrt(orbitals * energies))).astype(jnp.bfloat16)
    polar = lax.all_to_all(
        polar_entries.reshape(entry_shape), "energy", split_axis=0, concat_axis=1, tiled=True
    )
    inner = jnp.einsum(
        "ij,ejk->eik", coulomb_block, polar, preferred_element_type=jnp.float32
    ).astype(jnp.bfloat16)
    second = jnp.einsum("eij,jk->eik", inner, coulomb_block, preferred_element_type=jnp.float32)
    third = jnp.einsum(
        "eij,ejk->eik", inner, second.astype(jnp.bfloat16), preferred_element_type=jnp.float32
    )
    screened = (coulomb_block.astype(jnp.float32)[None] + second + third).astype(jnp.bfloat16)
    screened_entries = lax.all_to_all(
        screened, "energy", split_axis=1, concat_axis=0, tiled=True
    ).reshape(energies, -1)
    screen_real, screen_imag = spectrum(screened_entries)
    sigma_entries = to_values(
        green_real * screen_real - green_imag * screen_imag,
        green_real * screen_imag + green_imag * screen_real,
    )
    sigma_entries = (sigma_entries * (0.2 / math.sqrt(energies))).astype(jnp.bfloat16)
    sigma = lax.all_to_all(
        sigma_entries.reshape(entry_shape), "energy", split_axis=0, concat_axis=1, tiled=True
    )
    interface = couple_cols.shape[1]
    last = orbitals - interface
    coupling = coupling_matrix(couple_cols[0], couple_vals[0])
    prev_green, previous = from_behind((own_green, coupling), "slab", 1)
    next_green = from_behind(own_green, "slab", -1)
    prev_corner = prev_green[:, last:, last:]
    next_corner = next_green[:, :interface, :interface]
    near_next = jnp.einsum(
        "ij,ejk->eik", coupling, next_corner, preferred_element_type=jnp.float32
    ).astype(jnp.bfloat16)
    near_prev = jnp.einsum(
        "ji,ejk->eik", previous, prev_corner, preferred_element_type=jnp.float32
    ).astype(jnp.bfloat16)
    right_part = (
        jnp.einsum("eij,kj->eik", near_next, coupling, preferred_element_type=jnp.float32)
        * inv_root
    )
    left_part = (
        jnp.einsum("eij,jk->eik", near_prev, previous, preferred_element_type=jnp.float32)
        * inv_root
    )
    total = sigma.astype(jnp.float32)
    total = total.at[:, last:, last:].add(right_part)
    total = total.at[:, :interface, :interface].add(left_part)
    total_b = total.astype(jnp.bfloat16)
    dressed = jnp.einsum(
        "eij,ejk->eik", own_green, total_b, preferred_element_type=jnp.float32
    ).astype(jnp.bfloat16)
    updated = (
        own_green
        + jnp.einsum("eij,ejk->eik", dressed, own_green, preferred_element_type=jnp.float32)
        * inv_root
    )
    return updated.astype(jnp.bfloat16)[:, None]


MESH = pl.DeviceIdType.MESH


def unit_blocks(unit, grid):
    odd = grid - 1
    paired = grid * odd // 2
    slot = unit // odd
    turn = unit % odd
    diagonal = unit // paired
    first = (turn + slot) % odd
    second = (turn + odd - slot) % odd
    lone = 1 - (slot + odd - 1) // odd
    row = lone * odd + (1 - lone) * first
    col = lone * turn + (1 - lone) * second
    corner = 2 * (unit - paired)
    row0 = diagonal * corner + (1 - diagonal) * row
    col0 = diagonal * corner + (1 - diagonal) * col
    row1 = diagonal * (corner + 1) + (1 - diagonal) * col
    col1 = diagonal * (corner + 1) + (1 - diagonal) * row
    return ((row0, col0), (row1, col1))


def fused_kernel(
    volume, slabs, grid, scale_polar, scale_sigma, inv_root,
    green_hbm, coulomb_hbm, cols_hbm, vals_hbm, out,
    green, coulomb, cols, vals,
    green_in, mirror, polar_out, polar_in, polar_more, matrix, inner, screened, screen_in, sigma_out, sigma_in,
    coupling, turned, next_corner, left_out, left_in, total,
    send_sem, recv_sem, wave_send, wave_recv, more_send, more_recv, slab_send, slab_recv, load_sem,
):
    loads = [
        pltpu.make_async_copy(source, target, load_sem.at[n])
        for n, (source, target) in enumerate(
            ((green_hbm, green), (coulomb_hbm, coulomb), (cols_hbm, cols), (vals_hbm, vals))
        )
    ]
    for load in loads:
        load.start()
    me = lax.axis_index("energy")
    slab = lax.axis_index("slab")
    size = green.shape[0] // grid
    last = green.shape[0] - size
    order = sorted(range(1, volume), key=lambda k: (-min(k, volume - k), k))
    has_prev = 1 - (slabs - 1 - slab + 0) // (slabs - 1)
    has_next = 1 - slab // (slabs - 1)
    paired = grid * (grid - 1) // 2
    diagonal = me // paired
    pairs = volume // 2
    side = lax.rem(slab, 2)
    unit_here = me // 2
    hosting = lax.rem(me, 2) == side
    zero_unit = 1 - (unit_here + pairs - 1) // pairs

    def peer_of(k):
        return lax.rem(me + k, volume)

    barrier = pltpu.get_barrier_semaphore()
    for k in range(1, volume):
        pl.semaphore_signal(barrier, inc=1, device_id=(peer_of(k), slab), device_id_type=MESH)

    @pl.when(slab > 0)
    def _():
        pl.semaphore_signal(barrier, inc=1, device_id=(me, slab - 1), device_id_type=MESH)

    @pl.when(slab < slabs - 1)
    def _():
        pl.semaphore_signal(barrier, inc=1, device_id=(me, slab + 1), device_id_type=MESH)

    pl.semaphore_wait(barrier, volume - 1 + has_prev + has_next)

    def block_of(ref, coords):
        row = pl.multiple_of(coords[0] * size, size)
        col = pl.multiple_of(coords[1] * size, size)
        return ref.at[pl.ds(row, size), pl.ds(col, size)]

    def remote(src, dst, phase, k, half):
        return pltpu.make_async_remote_copy(
            src_ref=src, dst_ref=dst,
            send_sem=send_sem.at[phase, k, half], recv_sem=recv_sem.at[phase, k, half],
            device_id=(peer_of(k), slab), device_id_type=MESH,
        )

    def scatter(source, landing, phase):
        copies = []
        for k in order:
            coords = unit_blocks(peer_of(k), grid)
            for half in range(2):
                copy = remote(block_of(source, coords[half]), landing.at[me, half], phase, k, half)
                copy.start()
                copies.append(copy)
        own = unit_blocks(me, grid)
        for half in range(2):
            landing[me, half] = block_of(source, own[half])[...]
        return copies

    def gather(source, landing, phase, half):
        copies = []
        for k in order:
            copy = remote(source.at[peer_of(k), half], landing.at[me, half], phase, k, half)
            copy.start()
            copies.append(copy)
        landing[me, half] = source[me, half]
        return copies

    def arrived(copies):
        for copy in copies:
            copy.wait_recv()

    def assemble(landing, target):
        for unit in range(volume):
            coords = unit_blocks(unit, grid)
            for half in range(2):
                row, col = coords[half]
                target[row * size:(row + 1) * size, col * size:(col + 1) * size] = landing[unit, half]

    loads[0].wait()
    sent = scatter(green, green_in, 0)
    corner_copy = pltpu.make_async_remote_copy(
        src_ref=green.at[pl.ds(0, size), pl.ds(0, size)], dst_ref=next_corner,
        send_sem=slab_send.at[0], recv_sem=slab_recv.at[0],
        device_id=(me, slab - has_prev), device_id_type=MESH,
    )
    left_copy = pltpu.make_async_remote_copy(
        src_ref=left_out, dst_ref=left_in,
        send_sem=slab_send.at[1], recv_sem=slab_recv.at[1],
        device_id=(me, slab + has_next), device_id_type=MESH,
    )

    @pl.when(slab > 0)
    def _():
        corner_copy.start()

    loads[2].wait()
    loads[3].wait()
    ids = cols[...]
    values = vals[...].astype(jnp.float32)
    columns = lax.broadcasted_iota(jnp.int32, (size, size), 1)
    summed = jnp.zeros((size, size), jnp.float32)
    for k in range(ids.shape[1]):
        summed += jnp.where(ids[:, k:k + 1] == columns, values[:, k:k + 1], jnp.float32(0.0))
    summed = summed.astype(jnp.bfloat16).astype(jnp.float32)
    coupling[...] = summed.astype(jnp.bfloat16)
    turned[...] = summed.T.astype(jnp.bfloat16)

    @pl.when(slab < slabs - 1)
    def _():
        near_prev = plain_dot(turned[...], green[last:, last:]).astype(jnp.bfloat16)
        left_out[...] = plain_dot(near_prev, coupling[...]) * inv_root
        left_copy.start()

    arrived(sent)
    everything = list(sent)
    rows_at_once = 16

    for half in range(2):
        other = diagonal * half + (1 - diagonal) * (1 - half)

        def flip(e, carry, half=half, other=other):
            mirror[e, half] = green_in[e, other].astype(jnp.float32).T
            return carry

        lax.fori_loop(0, volume, flip, 0)

    def polar_copy(unit, half, piece):
        return pltpu.make_async_remote_copy(
            src_ref=piece, dst_ref=polar_in.at[me, half],
            send_sem=send_sem.at[1, unit, half], recv_sem=recv_sem.at[1, me, half],
            device_id=(2 * unit + side, slab), device_id_type=MESH,
        )

    def more_copy(half):
        return pltpu.make_async_remote_copy(
            src_ref=polar_out.at[half * pairs, 1], dst_ref=polar_more.at[me - paired, half],
            send_sem=more_send.at[half], recv_sem=more_recv.at[me - paired, half],
            device_id=(side, slab), device_id_type=MESH,
        )

    def polar_piece(unit, half):
        return polar_out.at[unit, half] if unit > 0 else polar_out.at[half * pairs, 0]

    for half in range(2):
        def correlate(step, carry, half=half):
            rows = pl.ds(pl.multiple_of(step * rows_at_once, rows_at_once), rows_at_once)
            mine = [green_in[e, half, rows, :].astype(jnp.float32) for e in range(volume)]
            theirs = [mirror[e, half, rows, :] for e in range(volume)]
            for e in range(pairs + 1):
                acc = mine[0] * theirs[(0 - e) % volume]
                for e2 in range(1, volume):
                    acc += mine[e2] * theirs[(e2 - e) % volume]
                polar_out[e, half, rows, :] = (acc * scale_polar).astype(jnp.bfloat16)
            return carry

        lax.fori_loop(0, size // rows_at_once, correlate, 0)
        for unit in range(pairs):
            ready = (half,) if unit > 0 else ((0, 1) if half == 0 else ())
            for part in ready:
                piece = polar_piece(unit, part)

                @pl.when(me != 2 * unit + side)
                def _(unit=unit, part=part, piece=piece):
                    polar_copy(unit, part, piece).start()

                @pl.when(me == 2 * unit + side)
                def _(part=part, piece=piece):
                    polar_in[me, part] = piece[...]

        if half == 1:
            @pl.when(me >= paired)
            def _():
                for part in range(2):
                    more_copy(part).start()

    other_energy = zero_unit * pairs + (1 - zero_unit) * (volume - unit_here)
    energies_here = (unit_here, other_energy)

    def wave_copy(which, k, half):
        coords = unit_blocks(peer_of(k), grid)[half]
        return pltpu.make_async_remote_copy(
            src_ref=block_of(screened.at[which], coords), dst_ref=screen_in.at[energies_here[which], half],
            send_sem=wave_send.at[which, k, half], recv_sem=wave_recv.at[energies_here[which], half],
            device_id=(peer_of(k), slab), device_id_type=MESH,
        )

    def send_waves(which, half):
        for k in order:
            wave_copy(which, k, half).start()
        own = unit_blocks(me, grid)[half]
        screen_in[energies_here[which], half] = block_of(screened.at[which], own)[...]

    def screen(which):
        inner[...] = plain_dot(coulomb[...], matrix[which]).astype(jnp.bfloat16)
        total[...] = plain_dot(inner[...], coulomb[...])
        matrix[which] = total[...].astype(jnp.bfloat16)
        third = plain_dot(inner[...], matrix[which])
        screened[which] = (coulomb[...].astype(jnp.float32) + total[...] + third).astype(jnp.bfloat16)

    def span(index):
        return slice(index * size, (index + 1) * size)

    def flipped(block):
        return block.astype(jnp.float32).T.astype(jnp.bfloat16)

    @pl.when(hosting)
    def _():
        for source in range(volume):
            @pl.when(me != source)
            def _(source=source):
                for half in range(2):
                    pltpu.make_async_remote_copy(
                        src_ref=polar_out.at[0, half], dst_ref=polar_in.at[source, half],
                        send_sem=send_sem.at[1, 0, half], recv_sem=recv_sem.at[1, source, half],
                        device_id=(source, slab), device_id_type=MESH,
                    ).wait_recv()

        @pl.when(unit_here == 0)
        def _():
            for source in range(volume - paired):
                for half in range(2):
                    pltpu.make_async_remote_copy(
                        src_ref=polar_out.at[0, half], dst_ref=polar_more.at[source, half],
                        send_sem=more_send.at[half], recv_sem=more_recv.at[source, half],
                        device_id=(source + paired, slab), device_id_type=MESH,
                    ).wait_recv()
            for which in range(2):
                for unit in range(volume):
                    (row0, col0), (row1, col1) = unit_blocks(unit, grid)
                    block = polar_in[unit, which]
                    matrix[which, span(row0), span(col0)] = block
                    matrix[which, span(row1), span(col1)] = (
                        flipped(block) if unit < paired else polar_more[unit - paired, which]
                    )

        @pl.when(unit_here > 0)
        def _():
            for unit in range(volume):
                for half in range(2):
                    row, col = unit_blocks(unit, grid)[half]
                    block = polar_in[unit, half]
                    matrix[0, span(row), span(col)] = block
                    matrix[1, span(col), span(row)] = flipped(block)

        loads[1].wait()
        screen(0)
        send_waves(0, 0)
        screen(1)
        send_waves(1, 0)
        send_waves(0, 1)
        send_waves(1, 1)

    @pl.when(lax.rem(me, 2) != side)
    def _():
        loads[1].wait()

    def waves_arrived(half):
        for e in range(volume):
            source = 2 * (0 if e == pairs else min(e, volume - e)) + side

            @pl.when(me != source)
            def _(e=e, source=source):
                pltpu.make_async_remote_copy(
                    src_ref=screen_in.at[e, half], dst_ref=screen_in.at[e, half],
                    send_sem=wave_send.at[0, 0, half], recv_sem=wave_recv.at[e, half],
                    device_id=(source, slab), device_id_type=MESH,
                ).wait_recv()

    sigma_copies = []
    for half in range(2):
        waves_arrived(half)

        def convolve(step, carry, half=half):
            rows = pl.ds(pl.multiple_of(step * rows_at_once, rows_at_once), rows_at_once)
            mine = [green_in[e, half, rows, :].astype(jnp.float32) for e in range(volume)]
            waves = [screen_in[e, half, rows, :].astype(jnp.float32) for e in range(volume)]
            for e in range(volume):
                acc = mine[0] * waves[e]
                for e2 in range(1, volume):
                    acc += mine[e2] * waves[(e - e2) % volume]
                sigma_out[e, half, rows, :] = (acc * scale_sigma).astype(jnp.bfloat16)
            return carry

        lax.fori_loop(0, size // rows_at_once, convolve, 0)
        sigma_copies += gather(sigma_out, sigma_in, 3, half)
    everything += sigma_copies
    arrived(sigma_copies)
    plane = matrix.at[0]
    assemble(sigma_in, plane)

    @pl.when(slab < slabs - 1)
    def _():
        corner_copy.wait_recv()
        near_next = plain_dot(coupling[...], next_corner[...]).astype(jnp.bfloat16)
        right_part = plain_dot(near_next, turned[...]) * inv_root
        plane[last:, last:] = (plane[last:, last:].astype(jnp.float32) + right_part).astype(jnp.bfloat16)
        left_copy.wait_send()

    @pl.when(slab > 0)
    def _():
        left_copy.wait_recv()
        plane[:size, :size] = (plane[:size, :size].astype(jnp.float32) + left_in[...]).astype(jnp.bfloat16)
        corner_copy.wait_send()

    inner[...] = plain_dot(green[...], plane[...]).astype(jnp.bfloat16)
    updated = green[...].astype(jnp.float32) + plain_dot(inner[...], green[...]) * inv_root
    out[...] = updated.astype(jnp.bfloat16)
    for copy in everything:
        copy.wait_send()
    for unit in range(pairs):
        @pl.when(me != 2 * unit + side)
        def _(unit=unit):
            for half in range(2):
                polar_copy(unit, half, polar_piece(unit, half)).wait_send()

    @pl.when(me >= paired)
    def _():
        for half in range(2):
            more_copy(half).wait_send()

    @pl.when(hosting)
    def _():
        for half in range(2):
            for which in range(2):
                for k in order:
                    wave_copy(which, k, half).wait_send()


def fused_on_device(grid, green_blocks, coulomb, couple_cols, couple_vals):
    volume = lax.axis_size("energy")
    slabs = lax.axis_size("slab")
    orbitals = green_blocks.shape[-1]
    size = orbitals // grid
    half_type = jnp.bfloat16
    pieces = pltpu.VMEM((volume, 2, size, size), half_type)
    whole = pltpu.VMEM((orbitals, orbitals), half_type)
    two = pltpu.VMEM((2, orbitals, orbitals), half_type)
    block = pltpu.VMEM((size, size), half_type)
    wide = pltpu.VMEM((size, size), jnp.float32)
    result = pl.pallas_call(
        functools.partial(
            fused_kernel, volume, slabs, grid,
            0.5 / math.sqrt(orbitals * volume), 0.2 / math.sqrt(volume), 1.0 / math.sqrt(orbitals),
        ),
        out_shape=jax.ShapeDtypeStruct((orbitals, orbitals), half_type),
        in_specs=[pl.BlockSpec(memory_space=pltpu.HBM)] * 4,
        out_specs=pl.BlockSpec(memory_space=pltpu.VMEM),
        scratch_shapes=[
            whole, whole, pltpu.VMEM(couple_cols.shape[1:], jnp.int32), pltpu.VMEM(couple_vals.shape[1:], half_type),
            pieces, pltpu.VMEM((volume, 2, size, size), jnp.float32), pieces, pieces,
            pltpu.VMEM((grid // 2, 2, size, size), half_type),
            two, whole, two, pieces, pieces, pieces,
            block, block, block, wide, wide, pltpu.VMEM((orbitals, orbitals), jnp.float32),
            pltpu.SemaphoreType.DMA((4, volume, 2)), pltpu.SemaphoreType.DMA((4, volume, 2)),
            pltpu.SemaphoreType.DMA((2, volume, 2)), pltpu.SemaphoreType.DMA((volume, 2)),
            pltpu.SemaphoreType.DMA((2,)), pltpu.SemaphoreType.DMA((grid // 2, 2)),
            pltpu.SemaphoreType.DMA((2,)), pltpu.SemaphoreType.DMA((2,)), pltpu.SemaphoreType.DMA((4,)),
        ],
        compiler_params=pltpu.CompilerParams(
            collective_id=0, has_side_effects=True, vmem_limit_bytes=40 * 2 ** 20
        ),
    )(green_blocks[0, 0], coulomb[0], couple_cols[0], couple_vals[0])
    return result[None, None]


def fused_grid(mesh):
    volume = mesh.shape["energy"]
    grid = math.isqrt(2 * volume)
    return grid if grid * grid == 2 * volume and grid % 2 == 0 else 0


def on_any(grid, green_blocks, coulomb, couple_cols, couple_vals):
    orbitals = green_blocks.shape[-1]
    fits = (
        grid > 0
        and green_blocks.shape[:2] == (1, 1)
        and orbitals % (128 * max(grid, 1)) == 0
        and couple_cols.shape[1] * grid == orbitals
        and lax.axis_size("slab") > 1
    )
    if fits:
        return fused_on_device(grid, green_blocks, coulomb, couple_cols, couple_vals)
    return on_device(green_blocks, coulomb, couple_cols, couple_vals)


def solution(mesh):
    return jax.shard_map(
        functools.partial(on_any, fused_grid(mesh)),
        mesh=mesh,
        in_specs=(
            P("energy", "slab", None, None),
            P("slab", None, None),
            P("slab", None, None),
            P("slab", None, None),
        ),
        out_specs=P("energy", "slab", None, None),
        check_vma=False,
    )
```

```python
import functools
import math

import jax
import jax.numpy as jnp
from jax import lax
from jax.experimental import pallas as pl
from jax.experimental.pallas import tpu as pltpu
from jax.sharding import PartitionSpec as P


def from_behind(x, axis, by):
    size = lax.axis_size(axis)
    pairs = [(i, i + by) for i in range(size) if 0 <= i + by < size]
    return lax.ppermute(x, axis, pairs)


def plain_dot(left, right):
    return jnp.dot(left, right, preferred_element_type=jnp.float32)


def split_parts(values):
    upper = values.astype(jnp.bfloat16)
    lower = (values - upper.astype(jnp.float32)).astype(jnp.bfloat16)
    return (upper, lower)


def coupling_matrix(column_ids, coupling_values):
    width = column_ids.shape[0]
    hits = column_ids[:, :, None] == jnp.arange(width, dtype=jnp.int32)[None, None, :]
    summed = jnp.sum(
        jnp.where(hits, coupling_values.astype(jnp.float32)[:, :, None], jnp.float32(0.0)), axis=1
    )
    return summed.astype(jnp.bfloat16)


def on_device(green_blocks, coulomb, couple_cols, couple_vals):
    own_green = green_blocks[:, 0]
    coulomb_block = coulomb[0]
    per_device = own_green.shape[0]
    orbitals = own_green.shape[1]
    volume = lax.axis_size("energy")
    energies = per_device * volume
    inv_root = 1.0 / math.sqrt(orbitals)
    flipped = jnp.swapaxes(own_green, 1, 2)
    received, flipped_recv = (
        lax.all_to_all(own_green, "energy", split_axis=1, concat_axis=0, tiled=True),
        lax.all_to_all(flipped, "energy", split_axis=1, concat_axis=0, tiled=True),
    )
    green_entries = received.reshape(energies, -1)
    flipped_entries = flipped_recv.reshape(energies, -1)
    entry_shape = received.shape
    halfway = energies // 2 + 1
    frequency = jnp.arange(halfway, dtype=jnp.int32)
    energy_index = jnp.arange(energies, dtype=jnp.int32)
    angles = (frequency[:, None] * energy_index[None, :] % energies).astype(jnp.float32) * (
        2.0 * math.pi / energies
    )
    cosine = jnp.cos(angles)
    sine = jnp.sin(angles)
    weights = (
        jnp.where((frequency == 0) | (2 * frequency == energies), 1.0, 2.0).astype(jnp.float32)
        / energies
    )
    forward_high, forward_low = split_parts(jnp.concatenate([cosine, -sine], axis=0))
    backward_table = jnp.concatenate(
        [cosine * weights[:, None], -sine * weights[:, None]], axis=0
    ).T
    backward_high, backward_low = split_parts(backward_table)

    def spectrum(entries):
        stacked = plain_dot(forward_high, entries) + plain_dot(forward_low, entries)
        return (stacked[:halfway], stacked[halfway:])

    def to_values(real_part, imag_part):
        data_high, data_low = split_parts(jnp.concatenate([real_part, imag_part], axis=0))
        return (
            plain_dot(backward_high, data_high)
            + plain_dot(backward_high, data_low)
            + plain_dot(backward_low, data_high)
        )

    green_real, green_imag = spectrum(green_entries)
    mirror_real, mirror_imag = spectrum(flipped_entries)
    polar_entries = to_values(
        green_real * mirror_real + green_imag * mirror_imag,
        green_imag * mirror_real - green_real * mirror_imag,
    )
    polar_entries = (polar_entries * (0.5 / math.sqrt(orbitals * energies))).astype(jnp.bfloat16)
    polar = lax.all_to_all(
        polar_entries.reshape(entry_shape), "energy", split_axis=0, concat_axis=1, tiled=True
    )
    inner = jnp.einsum(
        "ij,ejk->eik", coulomb_block, polar, preferred_element_type=jnp.float32
    ).astype(jnp.bfloat16)
    second = jnp.einsum("eij,jk->eik", inner, coulomb_block, preferred_element_type=jnp.float32)
    third = jnp.einsum(
        "eij,ejk->eik", inner, second.astype(jnp.bfloat16), preferred_element_type=jnp.float32
    )
    screened = (coulomb_block.astype(jnp.float32)[None] + second + third).astype(jnp.bfloat16)
    screened_entries = lax.all_to_all(
        screened, "energy", split_axis=1, concat_axis=0, tiled=True
    ).reshape(energies, -1)
    screen_real, screen_imag = spectrum(screened_entries)
    sigma_entries = to_values(
        green_real * screen_real - green_imag * screen_imag,
        green_real * screen_imag + green_imag * screen_real,
    )
    sigma_entries = (sigma_entries * (0.2 / math.sqrt(energies))).astype(jnp.bfloat16)
    sigma = lax.all_to_all(
        sigma_entries.reshape(entry_shape), "energy", split_axis=0, concat_axis=1, tiled=True
    )
    interface = couple_cols.shape[1]
    last = orbitals - interface
    coupling = coupling_matrix(couple_cols[0], couple_vals[0])
    prev_green, previous = from_behind((own_green, coupling), "slab", 1)
    next_green = from_behind(own_green, "slab", -1)
    prev_corner = prev_green[:, last:, last:]
    next_corner = next_green[:, :interface, :interface]
    near_next = jnp.einsum(
        "ij,ejk->eik", coupling, next_corner, preferred_element_type=jnp.float32
    ).astype(jnp.bfloat16)
    near_prev = jnp.einsum(
        "ji,ejk->eik", previous, prev_corner, preferred_element_type=jnp.float32
    ).astype(jnp.bfloat16)
    right_part = (
        jnp.einsum("eij,kj->eik", near_next, coupling, preferred_element_type=jnp.float32)
        * inv_root
    )
    left_part = (
        jnp.einsum("eij,jk->eik", near_prev, previous, preferred_element_type=jnp.float32)
        * inv_root
    )
    total = sigma.astype(jnp.float32)
    total = total.at[:, last:, last:].add(right_part)
    total = total.at[:, :interface, :interface].add(left_part)
    total_b = total.astype(jnp.bfloat16)
    dressed = jnp.einsum(
        "eij,ejk->eik", own_green, total_b, preferred_element_type=jnp.float32
    ).astype(jnp.bfloat16)
    updated = (
        own_green
        + jnp.einsum("eij,ejk->eik", dressed, own_green, preferred_element_type=jnp.float32)
        * inv_root
    )
    return updated.astype(jnp.bfloat16)[:, None]


MESH = pl.DeviceIdType.MESH


def unit_blocks(unit, grid):
    odd = grid - 1
    paired = grid * odd // 2
    slot = unit // odd
    turn = unit % odd
    diagonal = unit // paired
    first = (turn + slot) % odd
    second = (turn + odd - slot) % odd
    lone = 1 - (slot + odd - 1) // odd
    row = lone * odd + (1 - lone) * first
    col = lone * turn + (1 - lone) * second
    corner = 2 * (unit - paired)
    row0 = diagonal * corner + (1 - diagonal) * row
    col0 = diagonal * corner + (1 - diagonal) * col
    row1 = diagonal * (corner + 1) + (1 - diagonal) * col
    col1 = diagonal * (corner + 1) + (1 - diagonal) * row
    return ((row0, col0), (row1, col1))


def fused_kernel(
    volume, slabs, grid, scale_polar, scale_sigma, inv_root,
    green_hbm, coulomb_hbm, cols_hbm, vals_hbm, out,
    green, coulomb, cols, vals,
    green_in, mirror, polar_out, polar_in, matrix, inner, screened, screen_in, sigma_out, sigma_in,
    coupling, turned, next_corner, left_out, left_in, right_in, total,
    send_sem, recv_sem, slab_send, slab_recv, load_sem,
):
    loads = [
        pltpu.make_async_copy(source, target, load_sem.at[n])
        for n, (source, target) in enumerate(
            ((green_hbm, green), (coulomb_hbm, coulomb), (cols_hbm, cols), (vals_hbm, vals))
        )
    ]
    for load in loads:
        load.start()
    me = lax.axis_index("energy")
    slab = lax.axis_index("slab")
    size = green.shape[0] // grid
    last = green.shape[0] - size
    order = sorted(range(1, volume), key=lambda k: (-min(k, volume - k), k))
    has_prev = 1 - (slabs - 1 - slab + 0) // (slabs - 1)
    has_next = 1 - slab // (slabs - 1)
    diagonal = me // (grid * (grid - 1) // 2)

    def peer_of(k):
        return lax.rem(me + k, volume)

    barrier = pltpu.get_barrier_semaphore()
    for k in range(1, volume):
        pl.semaphore_signal(barrier, inc=1, device_id=(peer_of(k), slab), device_id_type=MESH)

    @pl.when(slab > 0)
    def _():
        pl.semaphore_signal(barrier, inc=1, device_id=(me, slab - 1), device_id_type=MESH)

    @pl.when(slab < slabs - 1)
    def _():
        pl.semaphore_signal(barrier, inc=1, device_id=(me, slab + 1), device_id_type=MESH)

    pl.semaphore_wait(barrier, volume - 1 + has_prev + has_next)

    def block_of(ref, coords):
        row = pl.multiple_of(coords[0] * size, size)
        col = pl.multiple_of(coords[1] * size, size)
        return ref.at[pl.ds(row, size), pl.ds(col, size)]

    def remote(src, dst, phase, k, half):
        return pltpu.make_async_remote_copy(
            src_ref=src, dst_ref=dst,
            send_sem=send_sem.at[phase, k, half], recv_sem=recv_sem.at[phase, k, half],
            device_id=(peer_of(k), slab), device_id_type=MESH,
        )

    def scatter(source, landing, phase):
        copies = []
        for half in range(2):
            for k in order:
                coords = unit_blocks(peer_of(k), grid)
                copy = remote(block_of(source, coords[half]), landing.at[me, half], phase, k, half)
                copy.start()
                copies.append(copy)
        own = unit_blocks(me, grid)
        for half in range(2):
            landing[me, half] = block_of(source, own[half])[...]
        return copies

    def gather(source, landing, phase, half):
        copies = []
        for k in order:
            copy = remote(source.at[peer_of(k), half], landing.at[me, half], phase, k, half)
            copy.start()
            copies.append(copy)
        landing[me, half] = source[me, half]
        return copies

    def arrived(copies):
        for copy in copies:
            copy.wait_recv()

    def from_of(k):
        return lax.rem(me + volume - k, volume)

    def place(landing, target, source, half):
        block_of(target, unit_blocks(source, grid)[half])[...] = landing[source, half]

    def assemble(landing, target, copies, half):
        place(landing, target, me, half)
        for k, copy in zip(order, copies):
            copy.wait_recv()
            place(landing, target, from_of(k), half)

    loads[0].wait()
    sent = scatter(green, green_in, 0)
    corner_copy = pltpu.make_async_remote_copy(
        src_ref=green.at[pl.ds(0, size), pl.ds(0, size)], dst_ref=next_corner,
        send_sem=slab_send.at[0], recv_sem=slab_recv.at[0],
        device_id=(me, slab - has_prev), device_id_type=MESH,
    )
    left_copy = pltpu.make_async_remote_copy(
        src_ref=left_out, dst_ref=left_in,
        send_sem=slab_send.at[1], recv_sem=slab_recv.at[1],
        device_id=(me, slab + has_next), device_id_type=MESH,
    )

    @pl.when(slab > 0)
    def _():
        corner_copy.start()

    loads[2].wait()
    loads[3].wait()
    ids = cols[...]
    values = vals[...].astype(jnp.float32)
    columns = lax.broadcasted_iota(jnp.int32, (size, size), 1)
    summed = jnp.zeros((size, size), jnp.float32)
    for k in range(ids.shape[1]):
        summed += jnp.where(ids[:, k:k + 1] == columns, values[:, k:k + 1], jnp.float32(0.0))
    summed = summed.astype(jnp.bfloat16).astype(jnp.float32)
    coupling[...] = summed.astype(jnp.bfloat16)
    turned[...] = summed.T.astype(jnp.bfloat16)

    @pl.when(slab < slabs - 1)
    def _():
        near_prev = plain_dot(turned[...], green[last:, last:]).astype(jnp.bfloat16)
        left_out[...] = plain_dot(near_prev, coupling[...]) * inv_root
        left_copy.start()

    everything = list(sent)
    rows_at_once = 16

    def flip(e, half):
        to = diagonal * half + (1 - diagonal) * (1 - half)
        mirror[e, to] = green_in[e, half].astype(jnp.float32).T

    for half in range(2):
        flip(me, half)
        for k, copy in zip(order, sent[half * len(order):]):
            copy.wait_recv()
            flip(from_of(k), half)

    polar_copies = []
    for half in range(2):
        def correlate(step, carry, half=half):
            rows = pl.ds(pl.multiple_of(step * rows_at_once, rows_at_once), rows_at_once)
            mine = [green_in[e, half, rows, :].astype(jnp.float32) for e in range(volume)]
            theirs = [mirror[e, half, rows, :] for e in range(volume)]
            for e in range(volume):
                acc = mine[0] * theirs[(0 - e) % volume]
                for e2 in range(1, volume):
                    acc += mine[e2] * theirs[(e2 - e) % volume]
                polar_out[e, half, rows, :] = (acc * scale_polar).astype(jnp.bfloat16)
            return carry

        lax.fori_loop(0, size // rows_at_once, correlate, 0)
        copies = gather(polar_out, polar_in, 1, half)
        everything += copies
        polar_copies.append(copies)
    loads[1].wait()
    for half in range(2):
        assemble(polar_in, matrix, polar_copies[half], half)
    inner[...] = plain_dot(coulomb[...], matrix[...]).astype(jnp.bfloat16)
    second = plain_dot(inner[...], coulomb[...])
    total[...] = second
    matrix[...] = second.astype(jnp.bfloat16)
    third = plain_dot(inner[...], matrix[...])
    screened[...] = (coulomb[...].astype(jnp.float32) + total[...] + third).astype(jnp.bfloat16)
    copies = scatter(screened, screen_in, 2)
    everything += copies
    waves = copies

    sigma_copies = []
    for half in range(2):
        arrived(waves[half * len(order):(half + 1) * len(order)])

        def convolve(step, carry, half=half):
            rows = pl.ds(pl.multiple_of(step * rows_at_once, rows_at_once), rows_at_once)
            mine = [green_in[e, half, rows, :].astype(jnp.float32) for e in range(volume)]
            waves = [screen_in[e, half, rows, :].astype(jnp.float32) for e in range(volume)]
            for e in range(volume):
                acc = mine[0] * waves[e]
                for e2 in range(1, volume):
                    acc += mine[e2] * waves[(e - e2) % volume]
                sigma_out[e, half, rows, :] = (acc * scale_sigma).astype(jnp.bfloat16)
            return carry

        lax.fori_loop(0, size // rows_at_once, convolve, 0)
        copies = gather(sigma_out, sigma_in, 3, half)
        everything += copies
        sigma_copies.append(copies)

    @pl.when(slab < slabs - 1)
    def _():
        corner_copy.wait_recv()
        near_next = plain_dot(coupling[...], next_corner[...]).astype(jnp.bfloat16)
        right_in[...] = plain_dot(near_next, turned[...]) * inv_root

    for half in range(2):
        assemble(sigma_in, matrix, sigma_copies[half], half)

    @pl.when(slab < slabs - 1)
    def _():
        matrix[last:, last:] = (matrix[last:, last:].astype(jnp.float32) + right_in[...]).astype(jnp.bfloat16)
        left_copy.wait_send()

    @pl.when(slab > 0)
    def _():
        left_copy.wait_recv()
        matrix[:size, :size] = (matrix[:size, :size].astype(jnp.float32) + left_in[...]).astype(jnp.bfloat16)
        corner_copy.wait_send()

    inner[...] = plain_dot(green[...], matrix[...]).astype(jnp.bfloat16)
    updated = green[...].astype(jnp.float32) + plain_dot(inner[...], green[...]) * inv_root
    out[...] = updated.astype(jnp.bfloat16)
    for copy in everything:
        copy.wait_send()


def fused_on_device(grid, green_blocks, coulomb, couple_cols, couple_vals):
    volume = lax.axis_size("energy")
    slabs = lax.axis_size("slab")
    orbitals = green_blocks.shape[-1]
    size = orbitals // grid
    half_type = jnp.bfloat16
    pieces = pltpu.VMEM((volume, 2, size, size), half_type)
    whole = pltpu.VMEM((orbitals, orbitals), half_type)
    block = pltpu.VMEM((size, size), half_type)
    wide = pltpu.VMEM((size, size), jnp.float32)
    result = pl.pallas_call(
        functools.partial(
            fused_kernel, volume, slabs, grid,
            0.5 / math.sqrt(orbitals * volume), 0.2 / math.sqrt(volume), 1.0 / math.sqrt(orbitals),
        ),
        out_shape=jax.ShapeDtypeStruct((orbitals, orbitals), half_type),
        in_specs=[pl.BlockSpec(memory_space=pltpu.HBM)] * 4,
        out_specs=pl.BlockSpec(memory_space=pltpu.VMEM),
        scratch_shapes=[
            whole, whole, pltpu.VMEM(couple_cols.shape[1:], jnp.int32), pltpu.VMEM(couple_vals.shape[1:], half_type),
            pieces, pltpu.VMEM((volume, 2, size, size), jnp.float32), pieces, pieces,
            whole, whole, whole, pieces, pieces, pieces,
            block, block, block, wide, wide, wide, pltpu.VMEM((orbitals, orbitals), jnp.float32),
            pltpu.SemaphoreType.DMA((4, volume, 2)), pltpu.SemaphoreType.DMA((4, volume, 2)),
            pltpu.SemaphoreType.DMA((2,)), pltpu.SemaphoreType.DMA((2,)), pltpu.SemaphoreType.DMA((4,)),
        ],
        compiler_params=pltpu.CompilerParams(
            collective_id=0, has_side_effects=True, vmem_limit_bytes=40 * 2 ** 20
        ),
    )(green_blocks[0, 0], coulomb[0], couple_cols[0], couple_vals[0])
    return result[None, None]


def fused_grid(mesh):
    volume = mesh.shape["energy"]
    grid = math.isqrt(2 * volume)
    return grid if grid * grid == 2 * volume and grid % 2 == 0 else 0


def on_any(grid, green_blocks, coulomb, couple_cols, couple_vals):
    orbitals = green_blocks.shape[-1]
    fits = (
        grid > 0
        and green_blocks.shape[:2] == (1, 1)
        and orbitals % (128 * max(grid, 1)) == 0
        and couple_cols.shape[1] * grid == orbitals
        and lax.axis_size("slab") > 1
    )
    if fits:
        return fused_on_device(grid, green_blocks, coulomb, couple_cols, couple_vals)
    return on_device(green_blocks, coulomb, couple_cols, couple_vals)


def solution(mesh):
    return jax.shard_map(
        functools.partial(on_any, fused_grid(mesh)),
        mesh=mesh,
        in_specs=(
            P("energy", "slab", None, None),
            P("slab", None, None),
            P("slab", None, None),
            P("slab", None, None),
        ),
        out_specs=P("energy", "slab", None, None),
        check_vma=False,
    )
```
